512 devices in a mesh: groups: 2 (over y), band: 64 (over z, core), chan: 4 (over x).
Axes of the slice: x: 4, y: 2, z: 32, core: 2. Of those that a mesh axis runs over, the one named last changes fastest.
The devices are a block of a 4x16x32 slice.
Arguments:
- slide_region: float32 [16, 512, 8192], P('chan', ('groups', 'band')), parts along dimension 1, may hold values from -6 to 6
- row_taps: float32 [16, 257], P('chan'), may hold values from -0.375 to 0.375
- column_taps: float32 [16, 257], replicated, may hold values from -0.375 to 0.375
- channel_mix: float32 [16, 16], replicated, may hold values from -1.5 to 1.5
Outputs:
- filtered: float32 [16, 512, 8192], P('chan', ('groups', 'band')), parts along dimension 1
The draws below stay inside these ranges and needn't reach their ends.
There are 2 independent parts, one for each index of `groups`. The reference program is written for one: setup_inputs(seed, part) draws one part's arguments, and reference() takes and returns one part's arrays. A program takes and returns all parts, laid end to end along the dimension named above; an argument that names none is the same for every part. Nothing has to cross between parts.
All inputs are finite; a program needn't handle non-finite values.
Results may differ from the reference program's by a relative error of at most 0.00007.
Values sent between devices are 32-bit elements; how exact they have to be, the bound alone decides.
A program may use at most 64 MiB of HBM per device.

```python
import jax
import jax.numpy as jnp
from jax import lax

C = 16
TAPS = 257
COLS = 8192
ROWS = 256


def block_scale(own_key, shape, split, least, largest):
    loudness, own = 1.0, jax.random.fold_in(own_key, 6)
    for axis_at, shards_of in split:
        draws = jnp.exp(jax.random.uniform(jax.random.fold_in(own, axis_at), (shards_of,), jnp.float32, least / len(split), largest / len(split)))
        loudness = loudness * jnp.repeat(draws, shape[axis_at] // shards_of).reshape([-1 if axis == axis_at else 1 for axis in range(len(shape))])
    return loudness


def scatter_about(own_key, shape, spread, reach, shards=(), dtype=jnp.bfloat16):
    loudness = block_scale(own_key, shape, shards, -0.22, 0.18) if shards else 1.0
    drawn = jax.random.normal(own_key, shape, jnp.float32) * spread * loudness
    return jnp.minimum(jnp.maximum(drawn, -reach), reach).astype(dtype)


def setup_inputs(seed: int = 0, part: int = 0) -> dict:
    arg_keys = jax.random.split(jax.random.key(seed), 5)
    part_splits = jax.random.split(jax.random.fold_in(arg_keys[4], part), 5)
    slide_region = scatter_about(part_splits[0], (C, ROWS, COLS), 1.0, 6.0, ((0, 4), (1, 64)), jnp.float32)
    row_taps = scatter_about(arg_keys[1], (C, TAPS), TAPS ** -0.5, 0.375, ((0, 4),), jnp.float32)
    column_taps = scatter_about(arg_keys[2], (C, TAPS), TAPS ** -0.5, 0.375, (), jnp.float32)
    channel_mix = scatter_about(arg_keys[3], (C, C), C ** -0.5, 1.5, (), jnp.float32)
    return dict(slide_region=slide_region, row_taps=row_taps, column_taps=column_taps, channel_mix=channel_mix)


def depthwise(signal, filter_taps, horizontal):
    channels = signal.shape[0]
    margin = (filter_taps.shape[1] - 1) // 2
    if horizontal:
        kernel = filter_taps[:, None, None, :]
        padding = ((0, 0), (margin, margin))
    else:
        kernel = filter_taps[:, None, :, None]
        padding = ((margin, margin), (0, 0))
    result = lax.conv_general_dilated(signal[None], kernel, (1, 1), padding,
                                      dimension_numbers=("NCHW", "OIHW", "NCHW"),
                                      feature_group_count=channels,
                                      precision=lax.Precision.HIGHEST)
    return result[0]


def reference(slide_region, row_taps, column_taps, channel_mix):
    across = depthwise(slide_region, row_taps, True)
    vertical = depthwise(across, column_taps, False)
    return jnp.einsum("oc,chw->ohw", channel_mix, vertical, precision=lax.Precision.HIGHEST)
```

```python
import functools

import jax
import jax.numpy as jnp
from jax import lax
from jax.experimental import pallas as pl
from jax.experimental.pallas import tpu as pltpu
from jax.sharding import PartitionSpec as P

MESH = pl.DeviceIdType.MESH
F32 = jnp.float32
BF16 = jnp.bfloat16
LANES = 128
HALF = 64


def two_parts(value):
    high = value.astype(BF16)
    low = (value - high.astype(F32)).astype(BF16)
    return high, low


def three_products(dot, left, right):
    (lh, ll), (rh, rl) = left, right
    return dot(lh, rh) + (dot(lh, rl) + dot(ll, rh))


def dot_nt(a, b):
    return lax.dot_general(a, b, (((1,), (1,)), ((), ())), preferred_element_type=F32)


def dot_nn(a, b):
    return lax.dot_general(a, b, (((1,), (0,)), ((), ())), preferred_element_type=F32)


def banded(row, count, width, shift):
    return pltpu.roll(jnp.broadcast_to(row, (count, width)), shift % width, 1, stride=1, stride_axis=0)


def kernel(
    bands, chans, x_ref, row_ref, col_ref, mix_ref, out_ref,
    taps, padded, row_high, row_low, sent, landed, col_high, col_low, coefs,
    gathered, mixed, returned,
    send_sems, recv_sems,
):
    me = lax.axis_index("band")
    my_z, my_core = me // 2, lax.rem(me, 2)
    my_x = lax.axis_index("chan")
    zs = bands // 2
    tiles = x_ref.shape[2] // LANES
    rows = x_ref.shape[1]
    height = bands * rows

    def band_peer(i):
        q, other = i // 2, lax.rem(i, 2)
        distance = zs // 2 - (q + 1) // 2
        z = lax.rem(my_z + distance * (2 * lax.rem(q, 2) - 1) + zs, zs)
        return z * 2 + lax.rem(my_core + other, 2)

    def chan_peer(j):
        return lax.rem(my_x + 1 + j, chans)

    barrier = pltpu.get_barrier_semaphore()

    def greet(i, _):
        pl.semaphore_signal(barrier, inc=1, device_id={"band": peer_of(i)}, device_id_type=MESH)
        return 0

    def peer_of(i):
        last = i // (bands - 2)
        return last * (me + 1 - 2 * my_core) + (1 - last) * band_peer(i)

    lax.fori_loop(0, bands - 1, greet, 0)
    for j in range(chans - 1):
        pl.semaphore_signal(barrier, inc=1, device_id={"chan": chan_peer(j)}, device_id_type=MESH)

    lane = lax.broadcasted_iota(jnp.int32, (1, 1, LANES), 2)
    left = lane < HALF
    sub = lax.broadcasted_iota(jnp.int32, (1, 2 * rows, 1), 1)
    upper = sub < rows

    taps[...] = jnp.zeros_like(taps)
    taps[0:4, 0:257] = row_ref[...]
    for c in range(4):
        table = banded(taps[c : c + 1, 0 : 3 * LANES], LANES, 3 * LANES, 0)
        high, low = two_parts(table)
        where = pl.ds((c % 2) * LANES, LANES)
        row_high[c // 2, where] = high
        row_low[c // 2, where] = low
    zero = jnp.zeros((2 * rows, LANES), F32)
    for p in range(2):
        padded[p, 0] = zero
        padded[p, tiles + 1] = zero
        for t in range(tiles):
            for c in range(2):
                padded[p, t + 1, c * rows : (c + 1) * rows] = x_ref[2 * p + c, :, t * LANES : (t + 1) * LANES]

    block = 16

    def filter_rows(n, _):
        t = n * block
        out = []
        for p in range(2):
            near = [padded[p, pl.ds(t + s, block)].reshape(block * 2 * rows, LANES) for s in range(3)]
            both = three_products(
                dot_nt, two_parts(jnp.concatenate(near, axis=1)), (row_high[p], row_low[p])
            )
            both = both.reshape(block, 2 * rows, 2 * LANES)
            out.append(jnp.where(upper, both[:, :, :LANES], both[:, :, LANES:]))
        sent[0, pl.ds(t, block)] = jnp.where(left, out[0], pltpu.roll(out[1], HALF, 2))
        sent[1, pl.ds(t, block)] = jnp.where(left, pltpu.roll(out[0], HALF, 2), out[1])
        return 0

    lax.fori_loop(0, tiles // block, filter_rows, 0)

    pl.semaphore_wait(barrier, bands - 1 + chans - 1)

    def out_to_bands(source, target, phase, k):
        def send(i, _):
            b = peer_of(i)
            pltpu.make_async_remote_copy(
                source.at[k, b], target.at[k, me], send_sems.at[phase, k], recv_sems.at[phase, k],
                device_id={"band": b}, device_id_type=MESH,
            ).start()
            return 0

        lax.fori_loop(0, bands - 1, send, 0)

    def all_bands(ref, sems, phase, k):
        view = ref.at[k, pl.ds(0, bands - 1)]
        pltpu.make_async_copy(view, view, sems.at[phase, k]).wait()

    def all_chans(sems, k):
        view = gathered.at[k, pl.ds(0, chans - 1)]
        pltpu.make_async_copy(view, view, sems.at[1, k]).wait()

    for k in range(2):
        out_to_bands(sent, landed, 0, k)
        landed[k, me] = sent[k, me]

    for c in range(4):
        taps[4:5, 0:257] = col_ref[pl.ds(my_x * 4 + c, 1), :]
        table = banded(taps[4:5, 0 : 2 * height], height, 2 * height, -(height // 2))[:, :height]
        high, low = two_parts(table)
        where = pl.ds((c // 2) * height, height)
        col_high[c % 2, where] = high
        col_low[c % 2, where] = low
    wide = lax.broadcasted_iota(jnp.int32, (8, LANES), 1) < HALF
    for o in range(2):
        for g in range(4 * chans // 2):
            first, second = 4 * (g // 2) + g % 2, 4 * (g // 2) + g % 2 + 2
            lo, hi = my_x * 4 + o, my_x * 4 + 2 + o
            coefs[o, g, 0] = jnp.where(wide, mix_ref[lo, first], mix_ref[hi, second])
            coefs[o, g, 1] = jnp.where(wide, mix_ref[lo, second], mix_ref[hi, first])

    for k in range(2):
        all_bands(landed, recv_sems, 0, k)
        tall = landed[k].reshape(bands // 2, 2, 2 * rows, LANES)
        even, odd = tall[:, 0], tall[:, 1]
        picked = (
            jnp.where(upper, even, pltpu.roll(odd, rows, 1)),
            jnp.where(upper, pltpu.roll(even, rows, 1), odd),
        )
        for c in range(2):
            signal = two_parts(picked[c].reshape(height, LANES))
            both = three_products(dot_nn, (col_high[c], col_low[c]), signal)
            gathered[k, my_x, c] = jnp.where(left[0], both[:height], both[height:])
        for j in range(chans - 1):
            pltpu.make_async_remote_copy(
                gathered.at[k, my_x], gathered.at[k, my_x], send_sems.at[1, k], recv_sems.at[1, k],
                device_id={"chan": chan_peer(j)}, device_id_type=MESH,
            ).start()
        all_chans(recv_sems, k)

        def mix_rows(n, _):
            total = [None, None]
            for g in range(2 * chans):
                value = gathered[k, g // 2, g % 2, pl.ds(pl.multiple_of(n * 8, 8), 8)]
                swapped = pltpu.roll(value, HALF, 1)
                for o in range(2):
                    term = coefs[o, g, 0] * value + coefs[o, g, 1] * swapped
                    total[o] = term if total[o] is None else total[o] + term
            first = upper[0]
            mixed[k, 2 * n] = jnp.where(first, total[0], pltpu.roll(total[1], rows, 0))
            mixed[k, 2 * n + 1] = jnp.where(first, pltpu.roll(total[0], rows, 0), total[1])
            return 0

        lax.fori_loop(0, height // 8, mix_rows, 0)
        out_to_bands(mixed, returned, 2, k)
        returned[k, me] = mixed[k, me]

    for k in range(2):
        all_bands(returned, recv_sems, 2, k)
    for t in range(tiles):
        a, b = returned[0, t], returned[1, t]
        keep = left[0]
        pair = (
            jnp.where(keep, a, pltpu.roll(b, HALF, 1)),
            jnp.where(keep, pltpu.roll(a, HALF, 1), b),
        )
        for p in range(2):
            for o in range(2):
                out_ref[2 * p + o, :, t * LANES : (t + 1) * LANES] = pair[p][o * rows : (o + 1) * rows]

    for k in range(2):
        all_bands(landed, send_sems, 0, k)
        all_chans(send_sems, k)
        all_bands(returned, send_sems, 2, k)


def on_device(bands, chans, slide_region, row_taps, column_taps, channel_mix):
    channels, rows, cols = slide_region.shape
    tiles = cols // LANES
    height = bands * rows
    vmem = pl.BlockSpec(memory_space=pltpu.VMEM)
    moved = pltpu.VMEM((2, bands, 2 * rows, LANES), F32)
    return pl.pallas_call(
        functools.partial(kernel, bands, chans),
        out_shape=jax.ShapeDtypeStruct(slide_region.shape, F32),
        in_specs=[vmem, vmem, vmem, pl.BlockSpec(memory_space=pltpu.SMEM)],
        out_specs=vmem,
        scratch_shapes=[
            pltpu.VMEM((8, 2 * height), F32),
            pltpu.VMEM((2, tiles + 2, 2 * rows, LANES), F32),
            pltpu.VMEM((2, 2 * LANES, 3 * LANES), BF16),
            pltpu.VMEM((2, 2 * LANES, 3 * LANES), BF16),
            moved,
            moved,
            pltpu.VMEM((2, 2 * height, height), BF16),
            pltpu.VMEM((2, 2 * height, height), BF16),
            pltpu.VMEM((2, 2 * chans, 2, 8, LANES), F32),
            pltpu.VMEM((2, chans, 2, height, LANES), F32),
            moved,
            moved,
            pltpu.SemaphoreType.DMA((3, 2)),
            pltpu.SemaphoreType.DMA((3, 2)),
        ],
        compiler_params=pltpu.CompilerParams(collective_id=0, has_side_effects=True),
    )(slide_region, row_taps, column_taps, channel_mix)


def solution(mesh):
    in_specs = (P("chan", ("groups", "band"), None), P("chan", None), P(), P())
    out_specs = P("chan", ("groups", "band"), None)
    return jax.shard_map(
        functools.partial(on_device, mesh.shape["band"], mesh.shape["chan"]),
        mesh=mesh, in_specs=in_specs, out_specs=out_specs, check_vma=False,
    )
```

```python
import functools

import jax
import jax.numpy as jnp
from jax import lax
from jax.experimental import pallas as pl
from jax.experimental.pallas import tpu as pltpu
from jax.sharding import PartitionSpec as P

MESH = pl.DeviceIdType.MESH
F32 = jnp.float32
BF16 = jnp.bfloat16
LANES = 128
HALF = 64


def two_parts(value):
    high = value.astype(BF16)
    low = (value - high.astype(F32)).astype(BF16)
    return high, low


def three_products(dot, left, right):
    (lh, ll), (rh, rl) = left, right
    return dot(lh, rh) + (dot(lh, rl) + dot(ll, rh))


def dot_nt(a, b):
    return lax.dot_general(a, b, (((1,), (1,)), ((), ())), preferred_element_type=F32)


def dot_nn(a, b):
    return lax.dot_general(a, b, (((1,), (0,)), ((), ())), preferred_element_type=F32)


def banded(row, count, width, shift):
    return pltpu.roll(jnp.broadcast_to(row, (count, width)), shift % width, 1, stride=1, stride_axis=0)


def kernel(
    bands, chans, x_hbm, row_hbm, col_hbm, mix_hbm, out_ref,
    x_ref, row_ref, col_ref, mix_ref, taps, padded, row_high, row_low, sent, landed, col_high, col_low, coefs,
    vertical, gathered, mixed, ordered, returned,
    send_sems, recv_sems, own_sems,
):
    fetches = [
        pltpu.make_async_copy(source, target, own_sems.at[n])
        for n, (source, target) in enumerate(
            ((row_hbm, row_ref), (x_hbm, x_ref), (col_hbm, col_ref), (mix_hbm, mix_ref))
        )
    ]
    for fetch in fetches:
        fetch.start()
    me = lax.axis_index("band")
    my_z, my_core = me // 2, lax.rem(me, 2)
    my_x = lax.axis_index("chan")
    zs = bands // 2
    tiles = x_ref.shape[2] // LANES
    rows = x_ref.shape[1]
    height = bands * rows

    half = zs // 2
    partner = me + 1 - 2 * my_core

    def around(distance):
        z = lax.rem(my_z + distance + zs, zs)
        return z * 2, z * 2 + 1

    def for_all_bands(act):
        for b in around(half):
            act(b)

        def step(n, _):
            for b in (*around(half - 1 - n), *around(n + 1 - half)):
                act(b)
            return 0

        lax.fori_loop(0, half - 1, step, 0)
        act(partner)

    group = zs // 2

    def for_groups(act):
        def step(n, _):
            first = n * group + lax.rem(my_z, group)

            @pl.when(first != my_z)
            def _():
                act(first * 2)
                act(first * 2 + 1)

            @pl.when(first == my_z)
            def _():
                act(partner)

            for away in range(1, group):
                z = n * group + lax.rem(my_z + away, group)
                act(z * 2)
                act(z * 2 + 1)
            return 0

        lax.fori_loop(0, zs // group, step, 0)

    def chan_peer(j):
        return lax.rem(my_x + 1 + j, chans)

    barrier = pltpu.get_barrier_semaphore()

    def greet_any(b):
        pl.semaphore_signal(barrier, inc=1, device_id={"band": b}, device_id_type=MESH)

    for_all_bands(greet_any)
    for j in range(chans - 1):
        pl.semaphore_signal(barrier, inc=1, device_id={"chan": chan_peer(j)}, device_id_type=MESH)

    lane = lax.broadcasted_iota(jnp.int32, (1, 1, LANES), 2)
    left = lane < HALF
    sub = lax.broadcasted_iota(jnp.int32, (1, 2 * rows, 1), 1)
    upper = sub < rows

    taps[...] = jnp.zeros_like(taps)
    fetches[0].wait()
    taps[0:4, 0:257] = row_ref[...]
    for c in range(4):
        table = banded(taps[c : c + 1, 0 : 3 * LANES], LANES, 3 * LANES, 0)
        high, low = two_parts(table)
        where = pl.ds((c % 2) * LANES, LANES)
        row_high[c // 2, where] = high
        row_low[c // 2, where] = low
    fetches[1].wait()
    zero = jnp.zeros((2 * rows, LANES), F32)
    for p in range(2):
        padded[p, 0] = zero
        padded[p, tiles + 1] = zero
        for t in range(tiles):
            for c in range(2):
                padded[p, t + 1, c * rows : (c + 1) * rows] = x_ref[2 * p + c, :, t * LANES : (t + 1) * LANES]

    block = 32

    def filter_rows(n, _):
        t = n * block
        out = []
        for p in range(2):
            near = [padded[p, pl.ds(t + s, block)].reshape(block * 2 * rows, LANES) for s in range(3)]
            both = three_products(
                dot_nt, two_parts(jnp.concatenate(near, axis=1)), (row_high[p], row_low[p])
            )
            both = both.reshape(block, 2 * rows, 2 * LANES)
            out.append(jnp.where(upper, both[:, :, :LANES], both[:, :, LANES:]))
        sent[0, pl.ds(t, block)] = jnp.where(left, out[0], pltpu.roll(out[1], HALF, 2))
        sent[1, pl.ds(t, block)] = jnp.where(left, pltpu.roll(out[0], HALF, 2), out[1])
        return 0

    lax.fori_loop(0, tiles // block, filter_rows, 0)

    pl.semaphore_wait(barrier, bands - 1 + chans - 1)

    def send(source, target, phase, k, b, at=None):
        pltpu.make_async_remote_copy(
            source.at[k, b if at is None else at], target.at[k, me], send_sems.at[phase, k], recv_sems.at[phase, k],
            device_id={"band": b}, device_id_type=MESH,
        ).start()

    for_all_bands(functools.partial(send, sent, landed, 0, 0))
    for_all_bands(functools.partial(send, sent, landed, 0, 1))
    for k in range(2):
        landed[k, me] = sent[k, me]

    fetches[2].wait()
    fetches[3].wait()
    for c in range(4):
        taps[4:5, 0:257] = col_ref[pl.ds(my_x * 4 + c, 1), :]
        table = banded(taps[4:5, 0 : 2 * height], height, 2 * height, -(height // 2))[:, :height]
        high, low = two_parts(table)
        where = pl.ds((c // 2) * height, height)
        col_high[c % 2, where] = high
        col_low[c % 2, where] = low
    wide = lax.broadcasted_iota(jnp.int32, (8, LANES), 1) < HALF
    for o in range(2 * chans):
        for g in range(2 * chans):
            first, second = 4 * (g // 2) + g % 2, 4 * (g // 2) + g % 2 + 2
            lo, hi = 4 * (o // 2) + o % 2, 4 * (o // 2) + o % 2 + 2
            coefs[o, g, 0] = jnp.where(wide, mix_ref[lo, first], mix_ref[hi, second])
            coefs[o, g, 1] = jnp.where(wide, mix_ref[lo, second], mix_ref[hi, first])

    runs = zs // chans
    def wait_bytes(ref, blocks, sem):
        view = ref.at[pl.ds(0, blocks)]
        pltpu.make_async_copy(view, view, sem).wait()

    def trade(source, target, phase, k):
        for j in range(chans - 1):
            x = chan_peer(j)
            pltpu.make_async_remote_copy(
                source.at[k, x], target.at[k, my_x], send_sems.at[phase, k], recv_sems.at[phase, k],
                device_id={"chan": x}, device_id_type=MESH,
            ).start()
        target[k, my_x] = source[k, my_x]
        wait_bytes(target.at[k], chans - 1, recv_sems.at[phase, k])

    for k in range(2):
        wait_bytes(landed.at[k], bands - 1, recv_sems.at[0, k])
        tall = landed[k].reshape(bands // 2, 2, 2 * rows, LANES)
        even, odd = tall[:, 0], tall[:, 1]
        picked = (
            jnp.where(upper, even, pltpu.roll(odd, rows, 1)),
            jnp.where(upper, pltpu.roll(even, rows, 1), odd),
        )
        for c in range(2):
            signal = two_parts(picked[c].reshape(height, LANES))
            both = three_products(dot_nn, (col_high[c], col_low[c]), signal)
            filtered = jnp.where(left[0], both[:height], both[height:])
            filtered = filtered.reshape(runs, chans, 2 * rows, LANES)
            for x in range(chans):
                vertical[k, x, c] = filtered[:, x]
        trade(vertical, gathered, 1, k)

        def mix_run(n, _):
            values = [gathered[k, g // 2, g % 2, n] for g in range(2 * chans)]
            swapped = [pltpu.roll(value, HALF, 1) for value in values]
            first = upper[0]
            for x in range(chans):
                total = [None, None]
                for o in range(2):
                    for g in range(2 * chans):
                        term = coefs[2 * x + o, g, 0] * values[g] + coefs[2 * x + o, g, 1] * swapped[g]
                        total[o] = term if total[o] is None else total[o] + term
                mixed[k, x, n, 0] = jnp.where(first, total[0], pltpu.roll(total[1], rows, 0))
                mixed[k, x, n, 1] = jnp.where(first, pltpu.roll(total[0], rows, 0), total[1])
            return 0

        lax.fori_loop(0, runs, mix_run, 0)

        trade(mixed, ordered, 3, k)

        def send_ordered(b):
            z, core = b // 2, lax.rem(b, 2)
            send(ordered.at[:, lax.rem(z, chans), z // chans], returned, 2, k, b, core)

        (for_all_bands, for_groups)[k](send_ordered)
        returned[k, me] = ordered[k, lax.rem(my_z, chans), my_z // chans, my_core]

    for k in range(2):
        wait_bytes(returned.at[k], bands - 1, recv_sems.at[2, k])
    for t in range(tiles):
        a, b = returned[0, t], returned[1, t]
        keep = left[0]
        pair = (
            jnp.where(keep, a, pltpu.roll(b, HALF, 1)),
            jnp.where(keep, pltpu.roll(a, HALF, 1), b),
        )
        for p in range(2):
            for o in range(2):
                out_ref[2 * p + o, :, t * LANES : (t + 1) * LANES] = pair[p][o * rows : (o + 1) * rows]

    for k in range(2):
        wait_bytes(landed.at[k], bands - 1, send_sems.at[0, k])
        wait_bytes(gathered.at[k], chans - 1, send_sems.at[1, k])
        wait_bytes(returned.at[k], bands - 1, send_sems.at[2, k])
        wait_bytes(ordered.at[k], chans - 1, send_sems.at[3, k])


def on_device(bands, chans, slide_region, row_taps, column_taps, channel_mix):
    channels, rows, cols = slide_region.shape
    tiles = cols // LANES
    height = bands * rows
    vmem = pl.BlockSpec(memory_space=pltpu.VMEM)
    runs = bands // 2 // chans
    traded = pltpu.VMEM((2, chans, 2, runs, 2 * rows, LANES), F32)
    results = pltpu.VMEM((2, chans, runs, 2, 2 * rows, LANES), F32)
    moved = pltpu.VMEM((2, bands, 2 * rows, LANES), F32)
    return pl.pallas_call(
        functools.partial(kernel, bands, chans),
        out_shape=jax.ShapeDtypeStruct(slide_region.shape, F32),
        in_specs=[pl.BlockSpec(memory_space=pl.ANY)] * 4,
        out_specs=vmem,
        scratch_shapes=[
            pltpu.VMEM(slide_region.shape, F32),
            pltpu.VMEM(row_taps.shape, F32),
            pltpu.VMEM(column_taps.shape, F32),
            pltpu.SMEM(channel_mix.shape, F32),
            pltpu.VMEM((8, 2 * height), F32),
            pltpu.VMEM((2, tiles + 2, 2 * rows, LANES), F32),
            pltpu.VMEM((2, 2 * LANES, 3 * LANES), BF16),
            pltpu.VMEM((2, 2 * LANES, 3 * LANES), BF16),
            moved,
            moved,
            pltpu.VMEM((2, 2 * height, height), BF16),
            pltpu.VMEM((2, 2 * height, height), BF16),
            pltpu.VMEM((2 * chans, 2 * chans, 2, 8, LANES), F32),
            traded,
            traded,
            results,
            results,
            moved,
            pltpu.SemaphoreType.DMA((4, 2)),
            pltpu.SemaphoreType.DMA((4, 2)),
            pltpu.SemaphoreType.DMA((4,)),
        ],
        compiler_params=pltpu.CompilerParams(collective_id=0, has_side_effects=True),
    )(slide_region, row_taps, column_taps, channel_mix)


def solution(mesh):
    in_specs = (P("chan", ("groups", "band"), None), P("chan", None), P(), P())
    out_specs = P("chan", ("groups", "band"), None)
    return jax.shard_map(
        functools.partial(on_device, mesh.shape["band"], mesh.shape["chan"]),
        mesh=mesh, in_specs=in_specs, out_specs=out_specs, check_vma=False,
    )
```

```python
import functools

import jax
import jax.numpy as jnp
from jax import lax
from jax.experimental import pallas as pl
from jax.experimental.pallas import tpu as pltpu
from jax.sharding import PartitionSpec as P

MESH = pl.DeviceIdType.MESH
F32 = jnp.float32
BF16 = jnp.bfloat16
LANES = 128
HALF = 64


def two_parts(value):
    high = value.astype(BF16)
    low = (value - high.astype(F32)).astype(BF16)
    return high, low


def three_products(dot, left, right):
    (lh, ll), (rh, rl) = left, right
    return dot(lh, rh) + (dot(lh, rl) + dot(ll, rh))


def dot_nt(a, b):
    return lax.dot_general(a, b, (((1,), (1,)), ((), ())), preferred_element_type=F32)


def dot_nn(a, b):
    return lax.dot_general(a, b, (((1,), (0,)), ((), ())), preferred_element_type=F32)


def banded(row, count, width, shift):
    return pltpu.roll(jnp.broadcast_to(row, (count, width)), shift % width, 1, stride=1, stride_axis=0)


def kernel(
    bands, chans, x_hbm, row_hbm, col_hbm, mix_hbm, out_hbm,
    x_ref, row_ref, col_ref, mix_ref, out_ref, taps, padded, row_high, row_low, sent, landed, col_high, col_low, coefs,
    vertical, gathered, mixed, ordered, returned,
    send_sems, recv_sems, own_sems,
):
    fetches = [
        pltpu.make_async_copy(source, target, own_sems.at[n])
        for n, (source, target) in enumerate(
            ((row_hbm, row_ref), (x_hbm, x_ref), (col_hbm, col_ref), (mix_hbm, mix_ref))
        )
    ]
    for fetch in fetches:
        fetch.start()
    me = lax.axis_index("band")
    my_z, my_core = me // 2, lax.rem(me, 2)
    my_x = lax.axis_index("chan")
    zs = bands // 2
    tiles = x_ref.shape[2] // LANES
    rows = x_ref.shape[1]
    height = bands * rows

    half = zs // 2
    partner = me + 1 - 2 * my_core

    def around(distance):
        z = lax.rem(my_z + distance + zs, zs)
        return z * 2, z * 2 + 1

    def for_all_bands(act):
        for b in around(half):
            act(b)

        def step(n, _):
            for b in (*around(half - 1 - n), *around(n + 1 - half)):
                act(b)
            return 0

        lax.fori_loop(0, half - 1, step, 0)
        act(partner)

    group = zs // 2

    def for_groups(act):
        def step(n, _):
            first = n * group + lax.rem(my_z, group)

            @pl.when(first != my_z)
            def _():
                act(first * 2)
                act(first * 2 + 1)

            @pl.when(first == my_z)
            def _():
                act(partner)

            for away in range(1, group):
                z = n * group + lax.rem(my_z + away, group)
                act(z * 2)
                act(z * 2 + 1)
            return 0

        lax.fori_loop(0, zs // group, step, 0)

    def chan_peer(j):
        return lax.rem(my_x + 1 + j, chans)

    barrier = pltpu.get_barrier_semaphore()

    def greet_any(b):
        pl.semaphore_signal(barrier, inc=1, device_id={"band": b}, device_id_type=MESH)

    for_all_bands(greet_any)
    for j in range(chans - 1):
        pl.semaphore_signal(barrier, inc=1, device_id={"chan": chan_peer(j)}, device_id_type=MESH)

    lane = lax.broadcasted_iota(jnp.int32, (1, 1, LANES), 2)
    left = lane < HALF
    sub = lax.broadcasted_iota(jnp.int32, (1, 2 * rows, 1), 1)
    upper = sub < rows

    taps[...] = jnp.zeros_like(taps)
    fetches[0].wait()
    taps[0:4, 0:257] = row_ref[...]
    for c in range(4):
        table = banded(taps[c : c + 1, 0 : 3 * LANES], LANES, 3 * LANES, 0)
        high, low = two_parts(table)
        where = pl.ds((c % 2) * LANES, LANES)
        row_high[c // 2, where] = high
        row_low[c // 2, where] = low
    fetches[1].wait()
    zero = jnp.zeros((2 * rows, LANES), F32)
    for p in range(2):
        padded[p, 0] = zero
        padded[p, tiles + 1] = zero
        for t in range(tiles):
            for c in range(2):
                padded[p, t + 1, c * rows : (c + 1) * rows] = x_ref[2 * p + c, :, t * LANES : (t + 1) * LANES]

    block = 32

    def filter_rows(n, _):
        t = n * block
        out = []
        for p in range(2):
            near = [padded[p, pl.ds(t + s, block)].reshape(block * 2 * rows, LANES) for s in range(3)]
            both = three_products(
                dot_nt, two_parts(jnp.concatenate(near, axis=1)), (row_high[p], row_low[p])
            )
            both = both.reshape(block, 2 * rows, 2 * LANES)
            out.append(jnp.where(upper, both[:, :, :LANES], both[:, :, LANES:]))
        sent[0, pl.ds(t, block)] = jnp.where(left, out[0], pltpu.roll(out[1], HALF, 2))
        sent[1, pl.ds(t, block)] = jnp.where(left, pltpu.roll(out[0], HALF, 2), out[1])
        return 0

    lax.fori_loop(0, tiles // block, filter_rows, 0)

    pl.semaphore_wait(barrier, bands - 1 + chans - 1)

    def send(source, target, phase, k, b, at=None):
        pltpu.make_async_remote_copy(
            source.at[k, b if at is None else at], target.at[k, me], send_sems.at[phase, k], recv_sems.at[phase, k],
            device_id={"band": b}, device_id_type=MESH,
        ).start()

    for_all_bands(functools.partial(send, sent, landed, 0, 0))
    for_all_bands(functools.partial(send, sent, landed, 0, 1))
    for k in range(2):
        landed[k, me] = sent[k, me]

    fetches[2].wait()
    fetches[3].wait()
    for c in range(4):
        taps[4:5, 0:257] = col_ref[pl.ds(my_x * 4 + c, 1), :]
        table = banded(taps[4:5, 0 : 2 * height], height, 2 * height, -(height // 2))[:, :height]
        high, low = two_parts(table)
        where = pl.ds((c // 2) * height, height)
        col_high[c % 2, where] = high
        col_low[c % 2, where] = low
    wide = lax.broadcasted_iota(jnp.int32, (8, LANES), 1) < HALF
    for o in range(2 * chans):
        for g in range(2 * chans):
            first, second = 4 * (g // 2) + g % 2, 4 * (g // 2) + g % 2 + 2
            lo, hi = 4 * (o // 2) + o % 2, 4 * (o // 2) + o % 2 + 2
            coefs[o, g, 0] = jnp.where(wide, mix_ref[lo, first], mix_ref[hi, second])
            coefs[o, g, 1] = jnp.where(wide, mix_ref[lo, second], mix_ref[hi, first])

    runs = zs // chans
    def wait_bytes(ref, blocks, sem):
        view = ref.at[pl.ds(0, blocks)]
        pltpu.make_async_copy(view, view, sem).wait()

    def trade(source, target, phase, k):
        for j in range(chans - 1):
            x = chan_peer(j)
            pltpu.make_async_remote_copy(
                source.at[k, x], target.at[k, my_x], send_sems.at[phase, k], recv_sems.at[phase, k],
                device_id={"chan": x}, device_id_type=MESH,
            ).start()
        target[k, my_x] = source[k, my_x]
        wait_bytes(target.at[k], chans - 1, recv_sems.at[phase, k])

    for k in range(2):
        wait_bytes(landed.at[k], bands - 1, recv_sems.at[0, k])
        tall = landed[k].reshape(bands // 2, 2, 2 * rows, LANES)
        even, odd = tall[:, 0], tall[:, 1]
        picked = (
            jnp.where(upper, even, pltpu.roll(odd, rows, 1)),
            jnp.where(upper, pltpu.roll(even, rows, 1), odd),
        )
        for c in range(2):
            signal = two_parts(picked[c].reshape(height, LANES))
            both = three_products(dot_nn, (col_high[c], col_low[c]), signal)
            filtered = jnp.where(left[0], both[:height], both[height:])
            filtered = filtered.reshape(runs, chans, 2 * rows, LANES)
            for x in range(chans):
                vertical[k, x, c] = filtered[:, x]
        trade(vertical, gathered, 1, k)

        def mix_run(n, _):
            values = [gathered[k, g // 2, g % 2, n] for g in range(2 * chans)]
            swapped = [pltpu.roll(value, HALF, 1) for value in values]
            first = upper[0]
            for x in range(chans):
                total = [None, None]
                for o in range(2):
                    for g in range(2 * chans):
                        term = coefs[2 * x + o, g, 0] * values[g] + coefs[2 * x + o, g, 1] * swapped[g]
                        total[o] = term if total[o] is None else total[o] + term
                mixed[k, x, n, 0] = jnp.where(first, total[0], pltpu.roll(total[1], rows, 0))
                mixed[k, x, n, 1] = jnp.where(first, pltpu.roll(total[0], rows, 0), total[1])
            return 0

        lax.fori_loop(0, runs, mix_run, 0)

        trade(mixed, ordered, 3, k)

        def send_ordered(b):
            z, core = b // 2, lax.rem(b, 2)
            send(ordered.at[:, lax.rem(z, chans), z // chans], returned, 2, k, b, core)

        (for_all_bands, for_groups)[k](send_ordered)
        returned[k, me] = ordered[k, lax.rem(my_z, chans), my_z // chans, my_core]

    for k in range(2):
        wait_bytes(returned.at[k], bands - 1, recv_sems.at[2, k])
    stores = []
    for t in range(tiles):
        a, b = returned[0, t], returned[1, t]
        keep = left[0]
        pair = (
            jnp.where(keep, a, pltpu.roll(b, HALF, 1)),
            jnp.where(keep, pltpu.roll(a, HALF, 1), b),
        )
        for p in range(2):
            for o in range(2):
                out_ref[2 * p + o, :, t * LANES : (t + 1) * LANES] = pair[p][o * rows : (o + 1) * rows]
        if (t + 1) % (tiles // 4) == 0:
            n = t // (tiles // 4)
            where = pl.ds(n * (tiles // 4) * LANES, (tiles // 4) * LANES)
            store = pltpu.make_async_copy(
                out_ref.at[:, :, where], out_hbm.at[:, :, where], own_sems.at[4 + n]
            )
            store.start()
            stores.append(store)

    for k in range(2):
        wait_bytes(landed.at[k], bands - 1, send_sems.at[0, k])
        wait_bytes(gathered.at[k], chans - 1, send_sems.at[1, k])
        wait_bytes(returned.at[k], bands - 1, send_sems.at[2, k])
        wait_bytes(ordered.at[k], chans - 1, send_sems.at[3, k])
    for store in stores:
        store.wait()


def on_device(bands, chans, slide_region, row_taps, column_taps, channel_mix):
    channels, rows, cols = slide_region.shape
    tiles = cols // LANES
    height = bands * rows
    runs = bands // 2 // chans
    traded = pltpu.VMEM((2, chans, 2, runs, 2 * rows, LANES), F32)
    results = pltpu.VMEM((2, chans, runs, 2, 2 * rows, LANES), F32)
    moved = pltpu.VMEM((2, bands, 2 * rows, LANES), F32)
    return pl.pallas_call(
        functools.partial(kernel, bands, chans),
        out_shape=jax.ShapeDtypeStruct(slide_region.shape, F32),
        in_specs=[pl.BlockSpec(memory_space=pl.ANY)] * 4,
        out_specs=pl.BlockSpec(memory_space=pl.ANY),
        scratch_shapes=[
            pltpu.VMEM(slide_region.shape, F32),
            pltpu.VMEM(row_taps.shape, F32),
            pltpu.VMEM(column_taps.shape, F32),
            pltpu.SMEM(channel_mix.shape, F32),
            pltpu.VMEM(slide_region.shape, F32),
            pltpu.VMEM((8, 2 * height), F32),
            pltpu.VMEM((2, tiles + 2, 2 * rows, LANES), F32),
            pltpu.VMEM((2, 2 * LANES, 3 * LANES), BF16),
            pltpu.VMEM((2, 2 * LANES, 3 * LANES), BF16),
            moved,
            moved,
            pltpu.VMEM((2, 2 * height, height), BF16),
            pltpu.VMEM((2, 2 * height, height), BF16),
            pltpu.VMEM((2 * chans, 2 * chans, 2, 8, LANES), F32),
            traded,
            traded,
            results,
            results,
            moved,
            pltpu.SemaphoreType.DMA((4, 2)),
            pltpu.SemaphoreType.DMA((4, 2)),
            pltpu.SemaphoreType.DMA((8,)),
        ],
        compiler_params=pltpu.CompilerParams(collective_id=0, has_side_effects=True),
    )(slide_region, row_taps, column_taps, channel_mix)


def solution(mesh):
    in_specs = (P("chan", ("groups", "band"), None), P("chan", None), P(), P())
    out_specs = P("chan", ("groups", "band"), None)
    return jax.shard_map(
        functools.partial(on_device, mesh.shape["band"], mesh.shape["chan"]),
        mesh=mesh, in_specs=in_specs, out_specs=out_specs, check_vma=False,
    )
```
